256 devices in a mesh: area: 32 (over y, x, core), rank: 8 (over z).
Axes of the slice: x: 4, y: 4, z: 8, core: 2. Of those that a mesh axis runs over, the one named last changes fastest.
Arguments:
- initial_bits: int32 [2, 48, 1024], P(None, None, ('area', 'rank')), may hold values from -2147483648 to 2147483646
- membrane: float32 [48, 32768], P(None, ('area', 'rank')), may hold values from -100 to 200
- drive: int32 [32768], P(('area', 'rank')), may hold values from 0 to 47
- leak_shift: int32 [32768], P(('area', 'rank')), may hold values from 2 to 5
- weights: bfloat16 [256, 128, 128, 128], P(('area', 'rank')), may hold values from -3 to 3, as said below
- pre_block: int32 [256, 128], P(('area', 'rank')), may hold values from 0 to 255
- block_mask: int32 [256, 128], P(('area', 'rank')), may hold values 0 or 1
- delay: int32 [256, 128], P(('area', 'rank')), may hold values from 2 to 5
- area_of_block: int32 [256, 1], replicated, may hold values from 0 to 31
Outputs:
- final_membrane: float32 [48, 32768], P(None, ('area', 'rank'))
- area_rates: float32 [10, 32], replicated
The draws below stay inside these ranges and needn't reach their ends.
Inputs may be any that keep to these rules, and one draw needn't show every extreme that they name: weights hold whole numbers. `area_of_block`: every area holds at least one block.
All inputs are finite; a program needn't handle non-finite values. No bound on the sum of `block_mask` on one device may be relied on, other than what follows from the above.
Results may differ from the reference program's by a relative error of at most 0.0003.
Values sent between devices are 32-bit elements; how exact they have to be, the bound alone decides.
A program may use at most 128 MiB of HBM per device.

```python
import jax
import jax.numpy as jnp
from jax import lax

BLOCK = 128
AREAS = 32
K = 128
TRIALS = 48
DMIN = 2
NDELAY = 4
STEPS = 10
BLOCKS = 256
NEURONS = 32768


def draw_weights(key, part):
    values = jax.random.randint(key, (BLOCKS, K, BLOCK, BLOCK), -3, 4)
    return values.astype(jnp.float32).astype(jnp.bfloat16)


def with_ends(result, stream_key, smallest, top_value):
    extent = result.shape
    index_at = [jax.random.randint(jax.random.fold_in(stream_key, axis), (), 0, extent[axis]) for axis in range(len(extent))]
    result = result.at[tuple(index_at)].set(smallest)
    longest = extent.index(max(extent))
    index_at[longest] = (index_at[longest] + 1) % extent[longest]
    return result.at[tuple(index_at)].set(top_value)


def block_levels(stream_key, shape, shards, smallest, largest):
    def one(position, shards_of):
        draws = jax.random.uniform(jax.random.fold_in(jax.random.fold_in(stream_key, 6), position), (shards_of,), jnp.float32, smallest / len(shards), largest / len(shards))
        return jnp.repeat(jnp.exp(draws), shape[position] // shards_of).reshape((-1,) + (1,) * (len(shape) - position - 1))

    gain = one(*shards[0])
    for cut in shards[1:]:
        gain = gain * one(*cut)
    return gain


def different_ones(own_key, rows, amount, top, lift):
    ranking = jax.random.permutation(jax.random.fold_in(own_key, 1), amount)
    favour = ranking
    for power in range(3):
        favour = favour * favour // amount
    favour = favour * lift // amount
    tickets = jax.random.randint(jax.random.fold_in(own_key, 2), (rows, amount), 0, 4096) + favour
    sure = jax.random.permutation(jax.random.fold_in(own_key, 3), rows)[jnp.arange(amount) % rows]
    tickets = jnp.where(jnp.arange(rows)[:, None] == sure[None, :], 1 << 14, tickets)
    merit = tickets * amount + jnp.arange(amount)
    return lax.top_k(merit.astype(jnp.int32), top)[1].astype(jnp.int32)


def setup_inputs(seed: int = 0) -> dict:
    arg_keys = jax.random.split(jax.random.key(seed), 10)
    initial_bits = with_ends(jax.random.randint(arg_keys[0], (DMIN, TRIALS, NEURONS // 32), -2147483648, 2147483647), jax.random.fold_in(arg_keys[0], 1), -2147483648, 2147483646).astype(jnp.int32)
    membrane = jnp.clip(-100.0 + 300.0 * jax.random.uniform(arg_keys[1], (TRIALS, NEURONS), jnp.float32) ** block_levels(arg_keys[1], (TRIALS, NEURONS), ((1, 256),), -0.2, 0.2), -100.0, 200.0)
    drive = with_ends(jax.random.randint(arg_keys[2], (NEURONS,), 0, 48), jax.random.fold_in(arg_keys[2], 1), 0, 47).astype(jnp.int32)
    leak_shift = with_ends(jax.random.randint(arg_keys[3], (NEURONS,), 2, 6), jax.random.fold_in(arg_keys[3], 1), 2, 5).astype(jnp.int32)
    weights = draw_weights(jax.random.fold_in(arg_keys[9], 71), 0)
    pre_block = with_ends(jax.random.randint(arg_keys[5], (BLOCKS, K), 0, BLOCKS), jax.random.fold_in(arg_keys[5], 1), 0, BLOCKS - 1).astype(jnp.int32)
    block_mask = with_ends((jax.random.randint(arg_keys[6], (BLOCKS, K), 0, 4) < 3).astype(jnp.int32), jax.random.fold_in(arg_keys[6], 1), 0, 1)
    delay = with_ends(jax.random.randint(arg_keys[7], (BLOCKS, K), DMIN, DMIN + NDELAY), jax.random.fold_in(arg_keys[7], 1), DMIN, (DMIN + NDELAY) - 1).astype(jnp.int32)
    area_of_block = different_ones(arg_keys[8], BLOCKS, AREAS, 1, 512)
    return dict(initial_bits=initial_bits, membrane=membrane, drive=drive, leak_shift=leak_shift, weights=weights, pre_block=pre_block, block_mask=block_mask, delay=delay, area_of_block=area_of_block)


threshold_level = 200.0


def unpack(packed):
    shifts = jnp.arange(32, dtype=jnp.int32)
    bit_values = jnp.bitwise_and(jnp.right_shift(packed[..., None], shifts), 1)
    return bit_values.reshape(packed.shape[:-1] + (packed.shape[-1] * 32,))


def reference(initial_bits, membrane, drive, leak_shift, weights, pre_block, block_mask, delay, area_of_block):
    neurons = BLOCKS * BLOCK
    intervals = STEPS // DMIN
    lag_table = (delay[:, :, None] - DMIN == jnp.arange(NDELAY, dtype=jnp.int32)[None, None, :]).astype(jnp.float32)
    input_weighting = block_mask.astype(jnp.float32)[:, :, None] * lag_table
    buffer = jnp.zeros((STEPS + NDELAY, TRIALS, neurons), jnp.float32)
    history = unpack(initial_bits).astype(jnp.float32)
    membrane_voltage = jnp.floor(membrane)
    leak_scale = 1.0 / jnp.left_shift(jnp.ones_like(leak_shift), leak_shift).astype(jnp.float32)
    drive_float = drive.astype(jnp.float32)
    area_table = (area_of_block[:, 0:1] == jnp.arange(AREAS, dtype=jnp.int32)[None, :]).astype(jnp.float32)
    block_counts = []
    for interval in range(intervals):
        source_rows = history.reshape(DMIN * TRIALS, BLOCKS, BLOCK)

        def one_block(operands):
            synapses, source, delay_weight_table = operands
            selected = jnp.take(source_rows, source, axis=1).astype(jnp.float32)
            product = jnp.einsum("rkm,kmn->krn", selected, synapses.astype(jnp.float32), precision=lax.Precision.HIGHEST)
            return jnp.einsum("kd,krn->drn", delay_weight_table, product, precision=lax.Precision.HIGHEST)

        arrived = lax.map(one_block, (weights, pre_block, input_weighting))
        arrived = arrived.reshape(BLOCKS, NDELAY, DMIN, TRIALS, BLOCK)
        arrived = jnp.transpose(arrived, (1, 2, 3, 0, 4)).reshape(NDELAY, DMIN, TRIALS, neurons)
        first_step = (interval - 1) * DMIN
        for lag_index in range(NDELAY):
            for offset in range(DMIN):
                landing = first_step + offset + DMIN + lag_index
                buffer = buffer.at[landing].add(arrived[lag_index, offset])
        fired_list = []
        for offset in range(DMIN):
            current = buffer[interval * DMIN + offset]
            membrane_voltage = membrane_voltage - jnp.floor(membrane_voltage * leak_scale) + current + drive_float
            current_spike_flags = membrane_voltage >= threshold_level
            membrane_voltage = jnp.where(current_spike_flags, jnp.zeros_like(membrane_voltage), jnp.maximum(membrane_voltage, -threshold_level))
            spikes = current_spike_flags.astype(jnp.float32)
            fired_list.append(spikes)
            block_counts.append(jnp.sum(spikes.reshape(TRIALS, BLOCKS, BLOCK), axis=(0, 2)))
        history = jnp.stack(fired_list)
    counts = jnp.dot(jnp.stack(block_counts), area_table, precision=lax.Precision.HIGHEST)
    sizes_per_area = jnp.sum(area_table, axis=0) * (TRIALS * BLOCK)
    return membrane_voltage, counts / sizes_per_area
```

```python
import functools

import jax
import jax.numpy as jnp
from jax import lax
from jax.experimental import pallas as pl
from jax.experimental.pallas import tpu as pltpu
from jax.sharding import PartitionSpec as P

AREAS = 32
DMIN = 2
STEPS = 10
THRESHOLD = 200.0
MESH = pl.DeviceIdType.MESH
WORDS = 3
SLOTS_PER_DOT = 4
NX, NY, NC = 4, 4, 2


def batches(nz):
    pairs = [(2 * near - 1, 2) for near in range(1, nz // 2 - 1)]
    return [(0, 1)] + pairs + [(nz - 3, 3)]


def z_place(offset, nz):
    return 2 * (nz - offset) if offset > nz // 2 else max(2 * offset - 1, 0)


def block_place(area, offset, areas, nz):
    place = jnp.where(offset > nz // 2, 2 * (nz - offset), jnp.maximum(2 * offset - 1, 0))
    first = jnp.where(place % 2 == 1, place, place - 1)
    count = jnp.where(place == 0, 1, 2)
    first = jnp.where(place == 0, 0, first)
    last = place >= nz - 3
    first = jnp.where(last, nz - 3, first)
    count = jnp.where(last, 3, count)
    return first * areas + area * count + place - first


def static_row(area, place, areas, nz):
    first, count = next(b for b in batches(nz) if b[0] <= place < b[0] + b[1])
    return (first * areas + area * count + place - first) * WORDS


def ring_hops(step, n):
    return min(step, n - step)


def plane_offsets(ny, nx, nc):
    found = [
        (dy, dx, dc)
        for dy in range(ny)
        for dx in range(nx)
        for dc in range(nc)
        if (dy, dx, dc) != (0, 0, 0)
    ]
    return sorted(found, key=lambda o: -(ring_hops(o[0], ny) + ring_hops(o[1], nx)))


def kernel(
    dims,
    pre_ref,
    mask_ref,
    delay_ref,
    bits_ref,
    membrane_ref,
    drive_ref,
    leak_ref,
    area_ref,
    weights_hbm,
    out_membrane,
    out_rates,
    weights,
    landing,
    words,
    volt,
    counts,
    tile,
    columns,
    totals,
    base0,
    base1,
    stride,
    odd,
    weights_sem,
    send_sem,
    z_sem,
    plane_sem,
    last_send_sem,
    last_z_sem,
    last_plane_sem,
):
    ny, nx, nc, nz, slots, trials, steps = dims
    areas = ny * nx * nc
    blocks = areas * nz
    per_interval = blocks * WORDS
    intervals = steps // DMIN
    area = lax.axis_index("area")
    rank = lax.axis_index("rank")
    y, x, core = area // (nx * nc), (area // nc) % nx, area % nc
    offsets = plane_offsets(ny, nx, nc)

    def plane_peer(offset):
        dy, dx, dc = offset
        there = (((y + dy) % ny) * nx + (x + dx) % nx) * nc + (core + dc) % nc
        return (there, rank)

    def z_peer(dz):
        return (area, (rank + dz) % nz)

    peers = [z_peer(dz) for dz in range(1, nz)] + [plane_peer(o) for o in offsets]
    barrier = pltpu.get_barrier_semaphore()
    for peer in peers:
        pl.semaphore_signal(barrier, inc=1, device_id=peer, device_id_type=MESH)

    load_weights = pltpu.make_async_copy(weights_hbm, weights, weights_sem)
    load_weights.start()

    def index_slot(k, carry):
        d, keep, pre = delay_ref[k], mask_ref[k], pre_ref[k]
        place = block_place(pre // nz, (pre % nz - rank + nz) % nz, areas, nz)
        base0[k] = keep * (((6 - d) // 2) * per_interval + place * WORDS)
        base1[k] = keep * (((7 - d) // 2) * per_interval + place * WORDS)
        stride[k] = keep * per_interval
        odd[k] = d % 2
        return carry

    lax.fori_loop(0, slots, index_slot, 0)

    def clear(j, carry):
        words[pl.ds(j * 8, 8)] = jnp.zeros((8, 1, 128), jnp.int32)
        return carry

    lax.fori_loop(0, 2 * per_interval // 8, clear, 0)
    counts[...] = jnp.zeros_like(counts)

    sublane = lax.broadcasted_iota(jnp.int32, (8, 128), 0)
    lane = lax.broadcasted_iota(jnp.int32, (trials, 128), 1)
    bit = [jnp.left_shift(jnp.int32(1), sublane + 8 * j) for j in range(4)]
    unscale = [1.0 / b.astype(jnp.float32) for b in bit]

    own_row = static_row(area, 0, areas, nz)

    def groups(fired):
        return [fired[8 * q : 8 * q + 8] for q in range(trials // 8)]

    def fold(parts):
        total = functools.reduce(jnp.bitwise_or, parts)
        return jnp.sum(total, axis=0, keepdims=True)

    def store_words(gather, first, second):
        first, second = groups(first), groups(second)
        zero = jnp.zeros((8, 128), jnp.int32)

        def take(flags, bits):
            return [jnp.where(f, b, zero) for f, b in zip(flags, bits)]

        row = own_row
        landing[gather, row] = fold(take(first[:4], bit))
        landing[gather, row + 1] = fold(take(first[4:], bit[:2]) + take(second[4:], bit[2:]))
        landing[gather, row + 2] = fold(take(second[:4], bit))

    def send(gather, row, count, device, there, semaphore):
        return pltpu.make_async_remote_copy(
            src_ref=landing.at[gather, pl.ds(row, count * WORDS)],
            dst_ref=landing.at[gather, pl.ds(there, count * WORDS)],
            send_sem=send_sem.at[gather],
            recv_sem=semaphore,
            device_id=device,
            device_id_type=MESH,
        )

    def exchange(gather):
        far_first = sorted(range(1, nz), key=lambda dz: -ring_hops(dz, nz))
        for dz in far_first:
            there = static_row(area, z_place(nz - dz, nz), areas, nz)
            send(gather, own_row, 1, z_peer(dz), there, z_sem.at[gather, dz - 1]).start()

        for number, (first, count) in enumerate(batches(nz)):
            for place in range(first, first + count):
                offset = next(o for o in range(nz) if z_place(o, nz) == place)
                if offset:
                    row = static_row(area, place, areas, nz)
                    semaphore = z_sem.at[gather, nz - offset - 1]
                    send(gather, row, 1, z_peer(offset), row, semaphore).wait_recv()
            row = static_row(area, first, areas, nz)
            for offset in offsets:
                send(
                    gather, row, count, plane_peer(offset), row, plane_sem.at[gather, number]
                ).start()

        for number, (first, count) in enumerate(batches(nz)):
            arrived = (areas - 1) * count
            send(gather, 0, arrived, z_peer(1), 0, plane_sem.at[gather, number]).wait_recv()
            rows = areas * count * WORDS
            start = areas * first * WORDS
            step = min(8, areas) * count * WORDS

            def keep(j, carry):
                at = start + j * step
                words[pl.ds((gather + 2) * per_interval + at, step)] = landing[
                    gather, pl.ds(at, step)
                ]
                return carry

            lax.fori_loop(0, rows // step, keep, 0)

    leak = leak_ref[...]
    scale = jnp.ones(leak.shape, jnp.float32)
    for power in range(5):
        on = jnp.bitwise_and(leak, 1 << power) != 0
        scale = scale * jnp.where(on, jnp.float32(2.0 ** -(1 << power)), jnp.float32(1.0))
    drive = drive_ref[...].astype(jnp.float32)
    volt[...] = jnp.floor(membrane_ref[...])

    def initial(step):
        packed = bits_ref[trials * step : trials * (step + 1)]
        spread_out = jnp.broadcast_to(packed[:, 0:1], (trials, 128))
        for w in range(1, 4):
            spread_out = jnp.where(
                lane >= 32 * w, jnp.broadcast_to(packed[:, w : w + 1], (trials, 128)), spread_out
            )
        picked = jnp.bitwise_and(jnp.right_shift(spread_out, jnp.bitwise_and(lane, 31)), 1)
        return picked != 0

    store_words(0, initial(0), initial(1))
    pl.semaphore_wait(barrier, len(peers))

    def lhs_of(k, interval):
        s = odd[k]
        row0 = base0[k] + interval * stride[k]
        row1 = base1[k] + interval * stride[k]
        w0 = words[row0 + 2 * s]
        w1 = jnp.right_shift(words[row0 + 1], 16 * s)
        w2 = words[row1 + 2 * (1 - s)]
        w3 = jnp.right_shift(words[row1 + 1], 16 * (1 - s))
        parts = []
        for wide, narrow in ((w0, w1), (w2, w3)):
            wide = jnp.broadcast_to(wide, (8, 128))
            narrow = jnp.broadcast_to(narrow, (8, 128))
            parts += [jnp.bitwise_and(wide, b) for b in bit]
            parts += [jnp.bitwise_and(narrow, b) for b in bit[: trials // 8 - 4]]
        return jnp.concatenate(parts, axis=0).astype(jnp.float32).astype(jnp.bfloat16)

    def one_interval(interval, carry):
        exchange(interval)

        @pl.when(interval == 0)
        def _():
            load_weights.wait()

        total = jnp.zeros((2 * trials, 128), jnp.float32)
        for first in range(0, slots, SLOTS_PER_DOT):
            spikes = jnp.concatenate(
                [lhs_of(first + j, interval) for j in range(SLOTS_PER_DOT)], axis=1
            )
            synapses = weights[first : first + SLOTS_PER_DOT].reshape(SLOTS_PER_DOT * 128, 128)
            total = total + jnp.dot(spikes, synapses, preferred_element_type=jnp.float32)
        half = unscale + unscale[: trials // 8 - 4]
        total = total * jnp.concatenate(half + half, axis=0)

        voltage = volt[...]
        fired = []
        for step in range(DMIN):
            voltage = (
                voltage
                - jnp.floor(voltage * scale)
                + total[trials * step : trials * (step + 1)]
                + drive
            )
            flags = voltage >= THRESHOLD
            voltage = jnp.where(flags, 0.0, jnp.maximum(voltage, -THRESHOLD))
            fired.append(flags)
        volt[...] = voltage

        @pl.when(interval < intervals - 1)
        def _():
            store_words(interval + 1, *fired)

        for step in range(DMIN):
            row = jnp.sum(fired[step].astype(jnp.float32), axis=0, keepdims=True)
            counts[pl.ds(interval * DMIN + step, 1), :] = row
        return carry

    lax.fori_loop(0, intervals, one_interval, 0)
    out_membrane[...] = volt[...]

    rows16 = lax.broadcasted_iota(jnp.int32, (16, 128), 0)
    lanes16 = lax.broadcasted_iota(jnp.int32, (16, 128), 1)
    per_step = jnp.broadcast_to(jnp.sum(counts[...], axis=1, keepdims=True), (16, 128))
    own = jnp.sum(jnp.where(rows16 == lanes16, per_step, 0.0), axis=0, keepdims=True)
    own = jnp.where(
        lax.broadcasted_iota(jnp.int32, (nz, 128), 0) == rank, jnp.broadcast_to(own, (nz, 128)), 0.0
    )
    tile[...] = own
    sends = []
    for dz in range(1, nz):
        copy = pltpu.make_async_remote_copy(
            src_ref=tile,
            dst_ref=columns.at[dz - 1],
            send_sem=last_send_sem.at[dz - 1],
            recv_sem=last_z_sem.at[dz - 1],
            device_id=z_peer(dz),
            device_id_type=MESH,
        )
        copy.start()
        sends.append(copy)
    whole = own
    for dz in range(1, nz):
        sends[dz - 1].wait_recv()
        whole = whole + columns[dz - 1]
    totals[area] = whole
    for number, offset in enumerate(offsets):
        copy = pltpu.make_async_remote_copy(
            src_ref=totals.at[area],
            dst_ref=totals.at[area],
            send_sem=last_send_sem.at[nz - 1 + number],
            recv_sem=last_plane_sem,
            device_id=plane_peer(offset),
            device_id_type=MESH,
        )
        copy.start()
        sends.append(copy)
    pltpu.make_async_remote_copy(
        src_ref=totals.at[pl.ds(0, len(offsets))],
        dst_ref=totals.at[pl.ds(0, len(offsets))],
        send_sem=last_send_sem.at[0],
        recv_sem=last_plane_sem,
        device_id=z_peer(1),
        device_id_type=MESH,
    ).wait_recv()

    by_block = totals[...].reshape(blocks, 128)
    table = (
        area_ref[...] == lax.broadcasted_iota(jnp.int32, (blocks, 128), 1)
    ).astype(jnp.float32)
    sizes = jnp.sum(table, axis=0, keepdims=True) * float(trials * 128)
    by_area = lax.dot_general(
        by_block,
        table,
        (((0,), (0,)), ((), ())),
        precision=lax.Precision.HIGHEST,
        preferred_element_type=jnp.float32,
    )
    rates = by_area / sizes
    out_rates[...] = rates[:steps, :AREAS]

    for copy in sends:
        copy.wait_send()

    sent = nz - 1 + len(offsets) * nz

    def drain(gather, carry):
        send(gather, 0, sent, z_peer(1), 0, z_sem.at[gather, 0]).wait_send()
        return carry

    lax.fori_loop(0, intervals, drain, 0)


def on_device(
    dims, initial_bits, membrane, drive, leak_shift, weights, pre_block, block_mask, delay, area_of_block
):
    ny, nx, nc, nz, slots, trials, steps = dims
    blocks = ny * nx * nc * nz
    intervals = steps // DMIN
    smem = pl.BlockSpec(memory_space=pltpu.SMEM)
    vmem = pl.BlockSpec(memory_space=pltpu.VMEM)
    run = pl.pallas_call(
        functools.partial(kernel, dims),
        out_shape=(
            jax.ShapeDtypeStruct((trials, 128), jnp.float32),
            jax.ShapeDtypeStruct((steps, AREAS), jnp.float32),
        ),
        in_specs=[smem] * 3 + [vmem] * 5 + [pl.BlockSpec(memory_space=pl.ANY)],
        out_specs=(vmem, vmem),
        scratch_shapes=[
            pltpu.VMEM((slots, 128, 128), jnp.bfloat16),
            pltpu.VMEM((intervals, blocks * WORDS, 1, 128), jnp.int32),
            pltpu.VMEM(((intervals + 2) * blocks * WORDS, 1, 128), jnp.int32),
            pltpu.VMEM((trials, 128), jnp.float32),
            pltpu.VMEM((16, 128), jnp.float32),
            pltpu.VMEM((nz, 128), jnp.float32),
            pltpu.VMEM((nz - 1, nz, 128), jnp.float32),
            pltpu.VMEM((ny * nx * nc, nz, 128), jnp.float32),
            pltpu.SMEM((slots,), jnp.int32),
            pltpu.SMEM((slots,), jnp.int32),
            pltpu.SMEM((slots,), jnp.int32),
            pltpu.SMEM((slots,), jnp.int32),
            pltpu.SemaphoreType.DMA,
            pltpu.SemaphoreType.DMA((intervals,)),
            pltpu.SemaphoreType.DMA((intervals, nz - 1)),
            pltpu.SemaphoreType.DMA((intervals, len(batches(nz)))),
            pltpu.SemaphoreType.DMA((nz - 1 + ny * nx * nc - 1,)),
            pltpu.SemaphoreType.DMA((nz - 1,)),
            pltpu.SemaphoreType.DMA,
        ],
        compiler_params=pltpu.CompilerParams(
            collective_id=0, has_side_effects=True, vmem_limit_bytes=32 << 20
        ),
    )
    return run(
        pre_block.reshape(slots),
        block_mask.reshape(slots),
        delay.reshape(slots),
        initial_bits.reshape(DMIN * trials, 4),
        membrane,
        drive.reshape(1, 128),
        leak_shift.reshape(1, 128),
        area_of_block,
        weights.reshape(slots, 128, 128),
    )


def build(mesh, dims):
    both = ("area", "rank")
    return jax.shard_map(
        functools.partial(on_device, dims),
        mesh=mesh,
        in_specs=(
            P(None, None, both),
            P(None, both),
            P(both),
            P(both),
            P(both, None, None, None),
            P(both, None),
            P(both, None),
            P(both, None),
            P(),
        ),
        out_specs=(P(None, both), P()),
        check_vma=False,
    )


def solution(mesh):
    return build(mesh, (NY, NX, NC, mesh.shape["rank"], 128, 48, STEPS))
```

```python
import functools

import jax
import jax.numpy as jnp
from jax import lax
from jax.experimental import pallas as pl
from jax.experimental.pallas import tpu as pltpu
from jax.sharding import PartitionSpec as P

AREAS = 32
DMIN = 2
STEPS = 10
THRESHOLD = 200.0
MESH = pl.DeviceIdType.MESH
WORDS = 3
SLOTS_PER_DOT = 4
NX, NY, NC = 4, 4, 2


def batches(nz):
    pairs = [(2 * near - 1, 2) for near in range(1, nz // 2 - 1)]
    return [(0, 1)] + pairs + [(nz - 3, 3)]


def z_place(offset, nz):
    return 2 * (nz - offset) if offset > nz // 2 else max(2 * offset - 1, 0)


def block_place(area, offset, areas, nz):
    place = jnp.where(offset > nz // 2, 2 * (nz - offset), jnp.maximum(2 * offset - 1, 0))
    first = jnp.where(place % 2 == 1, place, place - 1)
    count = jnp.where(place == 0, 1, 2)
    first = jnp.where(place == 0, 0, first)
    last = place >= nz - 3
    first = jnp.where(last, nz - 3, first)
    count = jnp.where(last, 3, count)
    return first * areas + area * count + place - first


def static_row(area, place, areas, nz):
    first, count = next(b for b in batches(nz) if b[0] <= place < b[0] + b[1])
    return (first * areas + area * count + place - first) * WORDS


def ring_hops(step, n):
    return min(step, n - step)


def plane_offsets(ny, nx, nc):
    found = [
        (dy, dx, dc)
        for dy in range(ny)
        for dx in range(nx)
        for dc in range(nc)
        if (dy, dx, dc) != (0, 0, 0)
    ]
    return sorted(found, key=lambda o: -(ring_hops(o[0], ny) + ring_hops(o[1], nx)))


def kernel(
    dims,
    pre_hbm,
    mask_hbm,
    delay_hbm,
    bits_hbm,
    membrane_hbm,
    drive_hbm,
    leak_hbm,
    area_hbm,
    weights_hbm,
    out_membrane,
    out_rates,
    pre_ref,
    mask_ref,
    delay_ref,
    bits_ref,
    membrane_ref,
    drive_ref,
    leak_ref,
    area_ref,
    weights,
    landing,
    words,
    volt,
    counts,
    tile,
    columns,
    totals,
    table_rows,
    table,
    input_sem,
    table_sem,
    weights_sem,
    send_sem,
    z_sem,
    plane_sem,
    last_send_sem,
    last_z_sem,
    last_plane_sem,
):
    ny, nx, nc, nz, slots, trials, steps = dims
    areas = ny * nx * nc
    blocks = areas * nz
    per_interval = blocks * WORDS
    intervals = steps // DMIN
    area = lax.axis_index("area")
    rank = lax.axis_index("rank")
    y, x, core = area // (nx * nc), (area // nc) % nx, area % nc
    offsets = plane_offsets(ny, nx, nc)

    def plane_peer(offset):
        dy, dx, dc = offset
        there = (((y + dy) % ny) * nx + (x + dx) % nx) * nc + (core + dc) % nc
        return (there, rank)

    def z_peer(dz):
        return (area, (rank + dz) % nz)

    peers = [z_peer(dz) for dz in range(1, nz)] + [plane_peer(o) for o in offsets]
    barrier = pltpu.get_barrier_semaphore()
    for peer in peers:
        pl.semaphore_signal(barrier, inc=1, device_id=peer, device_id_type=MESH)

    inputs = [
        (pre_hbm, pre_ref),
        (mask_hbm, mask_ref),
        (delay_hbm, delay_ref),
        (bits_hbm, bits_ref),
        (membrane_hbm, membrane_ref),
        (drive_hbm, drive_ref),
        (leak_hbm, leak_ref),
        (area_hbm, area_ref),
    ]
    loads = [
        pltpu.make_async_copy(source, target, input_sem.at[number])
        for number, (source, target) in enumerate(inputs)
    ]
    for load in loads:
        load.start()
    load_weights = pltpu.make_async_copy(weights_hbm, weights, weights_sem)
    load_weights.start()

    def clear(j, carry):
        words[pl.ds(j * 8, 8)] = jnp.zeros((8, 1, 128), jnp.int32)
        return carry

    lax.fori_loop(0, 2 * per_interval // 8, clear, 0)
    counts[...] = jnp.zeros_like(counts)
    for load in loads:
        load.wait()

    pre, keep_slot, d = pre_ref[...], mask_ref[...], delay_ref[...]
    place = block_place(pre // nz, (pre % nz - rank + nz) % nz, areas, nz)
    table_rows[0:1] = keep_slot * (((6 - d) // 2) * per_interval + place * WORDS)
    table_rows[1:2] = keep_slot * (((7 - d) // 2) * per_interval + place * WORDS)
    table_rows[2:3] = keep_slot * per_interval
    table_rows[3:4] = d % 2
    load_table = pltpu.make_async_copy(table_rows, table, table_sem)
    load_table.start()

    sublane = lax.broadcasted_iota(jnp.int32, (8, 128), 0)
    lane = lax.broadcasted_iota(jnp.int32, (trials, 128), 1)
    bit = [jnp.left_shift(jnp.int32(1), sublane + 8 * j) for j in range(4)]
    unscale = [1.0 / b.astype(jnp.float32) for b in bit]

    own_row = static_row(area, 0, areas, nz)

    def groups(fired):
        return [fired[8 * q : 8 * q + 8] for q in range(trials // 8)]

    def fold(parts):
        total = functools.reduce(jnp.bitwise_or, parts)
        return jnp.sum(total, axis=0, keepdims=True)

    def store_words(gather, first, second):
        first, second = groups(first), groups(second)
        zero = jnp.zeros((8, 128), jnp.int32)

        def take(flags, bits):
            return [jnp.where(f, b, zero) for f, b in zip(flags, bits)]

        row = own_row
        landing[gather, row] = fold(take(first[:4], bit))
        landing[gather, row + 1] = fold(take(first[4:], bit[:2]) + take(second[4:], bit[2:]))
        landing[gather, row + 2] = fold(take(second[:4], bit))

    def send(gather, row, count, device, there, semaphore):
        return pltpu.make_async_remote_copy(
            src_ref=landing.at[gather, pl.ds(row, count * WORDS)],
            dst_ref=landing.at[gather, pl.ds(there, count * WORDS)],
            send_sem=send_sem.at[gather],
            recv_sem=semaphore,
            device_id=device,
            device_id_type=MESH,
        )

    def exchange(gather):
        far_first = sorted(range(1, nz), key=lambda dz: -ring_hops(dz, nz))
        for dz in far_first:
            there = static_row(area, z_place(nz - dz, nz), areas, nz)
            send(gather, own_row, 1, z_peer(dz), there, z_sem.at[gather, dz - 1]).start()

        for number, (first, count) in enumerate(batches(nz)):
            for place in range(first, first + count):
                offset = next(o for o in range(nz) if z_place(o, nz) == place)
                if offset:
                    row = static_row(area, place, areas, nz)
                    semaphore = z_sem.at[gather, nz - offset - 1]
                    send(gather, row, 1, z_peer(offset), row, semaphore).wait_recv()
            row = static_row(area, first, areas, nz)
            for offset in offsets:
                send(
                    gather, row, count, plane_peer(offset), row, plane_sem.at[gather, number]
                ).start()

        for number, (first, count) in enumerate(batches(nz)):
            arrived = (areas - 1) * count
            send(gather, 0, arrived, z_peer(1), 0, plane_sem.at[gather, number]).wait_recv()
            rows = areas * count * WORDS
            start = areas * first * WORDS
            step = min(8, areas) * count * WORDS

            def keep(j, carry):
                at = start + j * step
                words[pl.ds((gather + 2) * per_interval + at, step)] = landing[
                    gather, pl.ds(at, step)
                ]
                return carry

            lax.fori_loop(0, rows // step, keep, 0)

    leak = leak_ref[...]
    scale = jnp.ones(leak.shape, jnp.float32)
    for power in range(5):
        on = jnp.bitwise_and(leak, 1 << power) != 0
        scale = scale * jnp.where(on, jnp.float32(2.0 ** -(1 << power)), jnp.float32(1.0))
    drive = drive_ref[...].astype(jnp.float32)
    volt[...] = jnp.floor(membrane_ref[...])

    def initial(step):
        packed = bits_ref[step]
        packed = jnp.concatenate([packed, jnp.zeros((4, trials), jnp.int32)], axis=0)
        packed = jnp.concatenate([packed, jnp.zeros((8, 128 - trials), jnp.int32)], axis=1)
        packed = jnp.transpose(packed)[:trials]
        spread_out = jnp.broadcast_to(packed[:, 0:1], (trials, 128))
        for w in range(1, 4):
            spread_out = jnp.where(
                lane >= 32 * w, jnp.broadcast_to(packed[:, w : w + 1], (trials, 128)), spread_out
            )
        picked = jnp.bitwise_and(jnp.right_shift(spread_out, jnp.bitwise_and(lane, 31)), 1)
        return picked != 0

    store_words(0, initial(0), initial(1))
    pl.semaphore_wait(barrier, len(peers))

    def lhs_of(k, interval):
        s = table[3, k]
        row0 = table[0, k] + interval * table[2, k]
        row1 = table[1, k] + interval * table[2, k]
        w0 = words[row0 + 2 * s]
        w1 = jnp.right_shift(words[row0 + 1], 16 * s)
        w2 = words[row1 + 2 * (1 - s)]
        w3 = jnp.right_shift(words[row1 + 1], 16 * (1 - s))
        parts = []
        for wide, narrow in ((w0, w1), (w2, w3)):
            wide = jnp.broadcast_to(wide, (8, 128))
            narrow = jnp.broadcast_to(narrow, (8, 128))
            parts += [jnp.bitwise_and(wide, b) for b in bit]
            parts += [jnp.bitwise_and(narrow, b) for b in bit[: trials // 8 - 4]]
        return jnp.concatenate(parts, axis=0).astype(jnp.float32).astype(jnp.bfloat16)

    def one_interval(interval, carry):
        exchange(interval)

        @pl.when(interval == 0)
        def _():
            load_weights.wait()
            load_table.wait()

        total = jnp.zeros((2 * trials, 128), jnp.float32)
        for first in range(0, slots, SLOTS_PER_DOT):
            spikes = jnp.concatenate(
                [lhs_of(first + j, interval) for j in range(SLOTS_PER_DOT)], axis=1
            )
            synapses = weights[first : first + SLOTS_PER_DOT].reshape(SLOTS_PER_DOT * 128, 128)
            total = total + jnp.dot(spikes, synapses, preferred_element_type=jnp.float32)
        half = unscale + unscale[: trials // 8 - 4]
        total = total * jnp.concatenate(half + half, axis=0)

        voltage = volt[...]
        fired = []
        for step in range(DMIN):
            voltage = (
                voltage
                - jnp.floor(voltage * scale)
                + total[trials * step : trials * (step + 1)]
                + drive
            )
            flags = voltage >= THRESHOLD
            voltage = jnp.where(flags, 0.0, jnp.maximum(voltage, -THRESHOLD))
            fired.append(flags)
        volt[...] = voltage

        @pl.when(interval < intervals - 1)
        def _():
            store_words(interval + 1, *fired)

        for step in range(DMIN):
            row = jnp.sum(fired[step].astype(jnp.float32), axis=0, keepdims=True)
            counts[pl.ds(interval * DMIN + step, 1), :] = row
        return carry

    lax.fori_loop(0, intervals, one_interval, 0)
    out_membrane[...] = volt[...]

    rows16 = lax.broadcasted_iota(jnp.int32, (16, 128), 0)
    lanes16 = lax.broadcasted_iota(jnp.int32, (16, 128), 1)
    per_step = jnp.broadcast_to(jnp.sum(counts[...], axis=1, keepdims=True), (16, 128))
    own = jnp.sum(jnp.where(rows16 == lanes16, per_step, 0.0), axis=0, keepdims=True)
    own = jnp.where(
        lax.broadcasted_iota(jnp.int32, (nz, 128), 0) == rank, jnp.broadcast_to(own, (nz, 128)), 0.0
    )
    tile[...] = own
    sends = []
    for dz in range(1, nz):
        copy = pltpu.make_async_remote_copy(
            src_ref=tile,
            dst_ref=columns.at[dz - 1],
            send_sem=last_send_sem.at[dz - 1],
            recv_sem=last_z_sem.at[dz - 1],
            device_id=z_peer(dz),
            device_id_type=MESH,
        )
        copy.start()
        sends.append(copy)
    whole = own
    for dz in range(1, nz):
        sends[dz - 1].wait_recv()
        whole = whole + columns[dz - 1]
    totals[area] = whole
    for number, offset in enumerate(offsets):
        copy = pltpu.make_async_remote_copy(
            src_ref=totals.at[area],
            dst_ref=totals.at[area],
            send_sem=last_send_sem.at[nz - 1 + number],
            recv_sem=last_plane_sem,
            device_id=plane_peer(offset),
            device_id_type=MESH,
        )
        copy.start()
        sends.append(copy)
    pltpu.make_async_remote_copy(
        src_ref=totals.at[pl.ds(0, len(offsets))],
        dst_ref=totals.at[pl.ds(0, len(offsets))],
        send_sem=last_send_sem.at[0],
        recv_sem=last_plane_sem,
        device_id=z_peer(1),
        device_id_type=MESH,
    ).wait_recv()

    by_block = totals[...].reshape(blocks, 128)
    area_row = jnp.broadcast_to(area_ref[...], (AREAS, blocks))
    belongs = (
        area_row == lax.broadcasted_iota(jnp.int32, (AREAS, blocks), 0)
    ).astype(jnp.float32)
    ones = jnp.ones((16, blocks), jnp.float32)
    sizes = lax.dot_general(
        ones,
        belongs,
        (((1,), (1,)), ((), ())),
        precision=lax.Precision.HIGHEST,
        preferred_element_type=jnp.float32,
    ) * float(trials * 128)
    by_area = lax.dot_general(
        jnp.transpose(by_block)[:16],
        belongs,
        (((1,), (1,)), ((), ())),
        precision=lax.Precision.HIGHEST,
        preferred_element_type=jnp.float32,
    )
    rates = by_area / sizes
    out_rates[...] = rates[:steps]

    for copy in sends:
        copy.wait_send()

    sent = nz - 1 + len(offsets) * nz

    def drain(gather, carry):
        send(gather, 0, sent, z_peer(1), 0, z_sem.at[gather, 0]).wait_send()
        return carry

    lax.fori_loop(0, intervals, drain, 0)


def on_device(
    dims, initial_bits, membrane, drive, leak_shift, weights, pre_block, block_mask, delay, area_of_block
):
    ny, nx, nc, nz, slots, trials, steps = dims
    blocks = ny * nx * nc * nz
    intervals = steps // DMIN
    hbm = pl.BlockSpec(memory_space=pl.ANY)
    vmem = pl.BlockSpec(memory_space=pltpu.VMEM)
    run = pl.pallas_call(
        functools.partial(kernel, dims),
        out_shape=(
            jax.ShapeDtypeStruct((trials, 128), jnp.float32),
            jax.ShapeDtypeStruct((steps, AREAS), jnp.float32),
        ),
        in_specs=[hbm] * 9,
        out_specs=(vmem, vmem),
        scratch_shapes=[
            pltpu.VMEM((1, slots), jnp.int32),
            pltpu.VMEM((1, slots), jnp.int32),
            pltpu.VMEM((1, slots), jnp.int32),
            pltpu.VMEM((DMIN, 4, trials), jnp.int32),
            pltpu.VMEM((trials, 128), jnp.float32),
            pltpu.VMEM((1, 128), jnp.int32),
            pltpu.VMEM((1, 128), jnp.int32),
            pltpu.VMEM((1, blocks), jnp.int32),
            pltpu.VMEM((slots, 128, 128), jnp.bfloat16),
            pltpu.VMEM((intervals, blocks * WORDS, 1, 128), jnp.int32),
            pltpu.VMEM(((intervals + 2) * blocks * WORDS, 1, 128), jnp.int32),
            pltpu.VMEM((trials, 128), jnp.float32),
            pltpu.VMEM((16, 128), jnp.float32),
            pltpu.VMEM((nz, 128), jnp.float32),
            pltpu.VMEM((nz - 1, nz, 128), jnp.float32),
            pltpu.VMEM((ny * nx * nc, nz, 128), jnp.float32),
            pltpu.VMEM((4, slots), jnp.int32),
            pltpu.SMEM((4, slots), jnp.int32),
            pltpu.SemaphoreType.DMA((8,)),
            pltpu.SemaphoreType.DMA,
            pltpu.SemaphoreType.DMA,
            pltpu.SemaphoreType.DMA((intervals,)),
            pltpu.SemaphoreType.DMA((intervals, nz - 1)),
            pltpu.SemaphoreType.DMA((intervals, len(batches(nz)))),
            pltpu.SemaphoreType.DMA((nz - 1 + ny * nx * nc - 1,)),
            pltpu.SemaphoreType.DMA((nz - 1,)),
            pltpu.SemaphoreType.DMA,
        ],
        compiler_params=pltpu.CompilerParams(
            collective_id=0, has_side_effects=True, vmem_limit_bytes=60 << 20
        ),
    )
    return run(
        pre_block,
        block_mask,
        delay,
        jnp.transpose(initial_bits, (0, 2, 1)),
        membrane,
        drive.reshape(1, 128),
        leak_shift.reshape(1, 128),
        area_of_block.reshape(1, blocks),
        weights.reshape(slots, 128, 128),
    )


def build(mesh, dims):
    both = ("area", "rank")
    return jax.shard_map(
        functools.partial(on_device, dims),
        mesh=mesh,
        in_specs=(
            P(None, None, both),
            P(None, both),
            P(both),
            P(both),
            P(both, None, None, None),
            P(both, None),
            P(both, None),
            P(both, None),
            P(),
        ),
        out_specs=(P(None, both), P()),
        check_vma=False,
    )


def solution(mesh):
    return build(mesh, (NY, NX, NC, mesh.shape["rank"], 128, 48, STEPS))
```

```python
import functools

import jax
import jax.numpy as jnp
from jax import lax
from jax.experimental import pallas as pl
from jax.experimental.pallas import tpu as pltpu
from jax.sharding import PartitionSpec as P

AREAS = 32
DMIN = 2
STEPS = 10
THRESHOLD = 200.0
MESH = pl.DeviceIdType.MESH
WORDS = 3
SLOTS_PER_DOT = 4
NX, NY, NC = 4, 4, 2


def batches(nz):
    pairs = [(2 * near - 1, 2) for near in range(1, nz // 2 - 1)]
    return [(0, 1)] + pairs + [(nz - 3, 3)]


def z_place(offset, nz):
    return 2 * (nz - offset) if offset > nz // 2 else max(2 * offset - 1, 0)


def block_place(area, offset, areas, nz):
    place = jnp.where(offset > nz // 2, 2 * (nz - offset), jnp.maximum(2 * offset - 1, 0))
    first = jnp.where(place % 2 == 1, place, place - 1)
    count = jnp.where(place == 0, 1, 2)
    first = jnp.where(place == 0, 0, first)
    last = place >= nz - 3
    first = jnp.where(last, nz - 3, first)
    count = jnp.where(last, 3, count)
    return first * areas + area * count + place - first


def static_row(area, place, areas, nz):
    first, count = next(b for b in batches(nz) if b[0] <= place < b[0] + b[1])
    return (first * areas + area * count + place - first) * WORDS


def ring_hops(step, n):
    return min(step, n - step)


def plane_offsets(ny, nx, nc):
    found = [
        (dy, dx, dc)
        for dy in range(ny)
        for dx in range(nx)
        for dc in range(nc)
        if (dy, dx, dc) != (0, 0, 0)
    ]
    return sorted(found, key=lambda o: -(ring_hops(o[0], ny) + ring_hops(o[1], nx)))


def kernel(
    dims,
    pre_hbm,
    mask_hbm,
    delay_hbm,
    bits_hbm,
    membrane_hbm,
    drive_hbm,
    leak_hbm,
    area_hbm,
    weights_hbm,
    out_membrane,
    out_rates,
    pre_ref,
    mask_ref,
    delay_ref,
    bits_ref,
    membrane_ref,
    drive_ref,
    leak_ref,
    area_ref,
    weights,
    landing,
    words,
    volt,
    counts,
    table_rows,
    table,
    input_sem,
    table_sem,
    weights_sem,
    send_sem,
    z_sem,
    plane_sem,
):
    ny, nx, nc, nz, slots, trials, steps = dims
    areas = ny * nx * nc
    blocks = areas * nz
    per_interval = blocks * WORDS
    intervals = steps // DMIN
    area = lax.axis_index("area")
    rank = lax.axis_index("rank")
    y, x, core = area // (nx * nc), (area // nc) % nx, area % nc
    offsets = plane_offsets(ny, nx, nc)

    def plane_peer(offset):
        dy, dx, dc = offset
        there = (((y + dy) % ny) * nx + (x + dx) % nx) * nc + (core + dc) % nc
        return (there, rank)

    def z_peer(dz):
        return (area, (rank + dz) % nz)

    peers = [z_peer(dz) for dz in range(1, nz)] + [plane_peer(o) for o in offsets]
    barrier = pltpu.get_barrier_semaphore()
    for peer in peers:
        pl.semaphore_signal(barrier, inc=1, device_id=peer, device_id_type=MESH)

    inputs = [
        (pre_hbm, pre_ref),
        (mask_hbm, mask_ref),
        (delay_hbm, delay_ref),
        (bits_hbm, bits_ref),
        (membrane_hbm, membrane_ref),
        (drive_hbm, drive_ref),
        (leak_hbm, leak_ref),
        (area_hbm, area_ref),
    ]
    loads = [
        pltpu.make_async_copy(source, target, input_sem.at[number])
        for number, (source, target) in enumerate(inputs)
    ]
    for load in loads:
        load.start()
    load_weights = pltpu.make_async_copy(weights_hbm, weights, weights_sem)
    load_weights.start()

    def clear(j, carry):
        words[pl.ds(j * 8, 8)] = jnp.zeros((8, 1, 128), jnp.int32)
        return carry

    lax.fori_loop(0, 2 * per_interval // 8, clear, 0)
    counts[...] = jnp.zeros_like(counts)
    for load in loads:
        load.wait()

    pre, keep_slot, d = pre_ref[...], mask_ref[...], delay_ref[...]
    place = block_place(pre // nz, (pre % nz - rank + nz) % nz, areas, nz)
    table_rows[0:1] = keep_slot * (((6 - d) // 2) * per_interval + place * WORDS)
    table_rows[1:2] = keep_slot * (((7 - d) // 2) * per_interval + place * WORDS)
    table_rows[2:3] = keep_slot * per_interval
    table_rows[3:4] = d % 2
    load_table = pltpu.make_async_copy(table_rows, table, table_sem)
    load_table.start()

    sublane = lax.broadcasted_iota(jnp.int32, (8, 128), 0)
    lane = lax.broadcasted_iota(jnp.int32, (trials, 128), 1)
    bit = [jnp.left_shift(jnp.int32(1), sublane + 8 * j) for j in range(4)]
    unscale = [1.0 / b.astype(jnp.float32) for b in bit]

    own_row = static_row(area, 0, areas, nz)

    def groups(fired):
        return [fired[8 * q : 8 * q + 8] for q in range(trials // 8)]

    def fold(parts):
        total = functools.reduce(jnp.bitwise_or, parts)
        return jnp.sum(total, axis=0, keepdims=True)

    def store_words(gather, first, second):
        first, second = groups(first), groups(second)
        zero = jnp.zeros((8, 128), jnp.int32)

        def take(flags, bits):
            return [jnp.where(f, b, zero) for f, b in zip(flags, bits)]

        row = own_row
        landing[gather, row] = fold(take(first[:4], bit))
        landing[gather, row + 1] = fold(take(first[4:], bit[:2]) + take(second[4:], bit[2:]))
        landing[gather, row + 2] = fold(take(second[:4], bit))

    def send(gather, row, count, device, there, semaphore):
        return pltpu.make_async_remote_copy(
            src_ref=landing.at[gather, pl.ds(row, count * WORDS)],
            dst_ref=landing.at[gather, pl.ds(there, count * WORDS)],
            send_sem=send_sem.at[gather],
            recv_sem=semaphore,
            device_id=device,
            device_id_type=MESH,
        )

    def exchange(gather):
        far_first = sorted(range(1, nz), key=lambda dz: -ring_hops(dz, nz))
        for dz in far_first:
            there = static_row(area, z_place(nz - dz, nz), areas, nz)
            send(gather, own_row, 1, z_peer(dz), there, z_sem.at[gather, dz - 1]).start()

        for number, (first, count) in enumerate(batches(nz)):
            for place in range(first, first + count):
                offset = next(o for o in range(nz) if z_place(o, nz) == place)
                if offset:
                    row = static_row(area, place, areas, nz)
                    semaphore = z_sem.at[gather, nz - offset - 1]
                    send(gather, row, 1, z_peer(offset), row, semaphore).wait_recv()
            row = static_row(area, first, areas, nz)
            for offset in offsets:
                send(
                    gather, row, count, plane_peer(offset), row, plane_sem.at[gather, number]
                ).start()

        for number, (first, count) in enumerate(batches(nz)):
            arrived = (areas - 1) * count
            send(gather, 0, arrived, z_peer(1), 0, plane_sem.at[gather, number]).wait_recv()
            rows = areas * count * WORDS
            start = areas * first * WORDS
            step = min(8, areas) * count * WORDS

            def keep(j, carry):
                at = start + j * step
                words[pl.ds((gather + 2) * per_interval + at, step)] = landing[
                    gather, pl.ds(at, step)
                ]
                return carry

            lax.fori_loop(0, rows // step, keep, 0)

    leak = leak_ref[...]
    scale = jnp.ones(leak.shape, jnp.float32)
    for power in range(5):
        on = jnp.bitwise_and(leak, 1 << power) != 0
        scale = scale * jnp.where(on, jnp.float32(2.0 ** -(1 << power)), jnp.float32(1.0))
    drive = drive_ref[...].astype(jnp.float32)
    volt[...] = jnp.floor(membrane_ref[...])

    def initial(step):
        packed = bits_ref[step]
        packed = jnp.concatenate([packed, jnp.zeros((4, trials), jnp.int32)], axis=0)
        packed = jnp.concatenate([packed, jnp.zeros((8, 128 - trials), jnp.int32)], axis=1)
        packed = jnp.transpose(packed)[:trials]
        spread_out = jnp.broadcast_to(packed[:, 0:1], (trials, 128))
        for w in range(1, 4):
            spread_out = jnp.where(
                lane >= 32 * w, jnp.broadcast_to(packed[:, w : w + 1], (trials, 128)), spread_out
            )
        picked = jnp.bitwise_and(jnp.right_shift(spread_out, jnp.bitwise_and(lane, 31)), 1)
        return picked != 0

    store_words(0, initial(0), initial(1))
    lane_area = lax.broadcasted_iota(jnp.int32, (128, blocks), 0) % AREAS
    belongs = (jnp.broadcast_to(area_ref[...], (128, blocks)) == lane_area).astype(jnp.float32)
    sizes = lax.dot_general(
        jnp.ones((8, blocks), jnp.float32),
        belongs,
        (((1,), (1,)), ((), ())),
        precision=lax.Precision.HIGHEST,
        preferred_element_type=jnp.float32,
    )[0:1] * float(trials * 128)
    block_lane = lax.broadcasted_iota(jnp.int32, (1, blocks), 1)
    own_area = jnp.sum(
        jnp.where(block_lane == area * nz + rank, area_ref[...], 0), axis=1, keepdims=True
    )
    lanes = lax.broadcasted_iota(jnp.int32, (1, 128), 1)
    own_lanes = lanes % AREAS == own_area
    pl.semaphore_wait(barrier, len(peers))
    exchange(0)
    load_weights.wait()
    load_table.wait()

    def lhs_of(k, interval):
        s = table[3, k]
        row0 = table[0, k] + interval * table[2, k]
        row1 = table[1, k] + interval * table[2, k]
        w0 = words[row0 + 2 * s]
        w1 = jnp.right_shift(words[row0 + 1], 16 * s)
        w2 = words[row1 + 2 * (1 - s)]
        w3 = jnp.right_shift(words[row1 + 1], 16 * (1 - s))
        parts = []
        for wide, narrow in ((w0, w1), (w2, w3)):
            wide = jnp.broadcast_to(wide, (8, 128))
            narrow = jnp.broadcast_to(narrow, (8, 128))
            parts += [jnp.bitwise_and(wide, b) for b in bit]
            parts += [jnp.bitwise_and(narrow, b) for b in bit[: trials // 8 - 4]]
        return jnp.concatenate(parts, axis=0).astype(jnp.float32).astype(jnp.bfloat16)

    def one_interval(interval, carry):
        total = jnp.zeros((2 * trials, 128), jnp.float32)
        for first in range(0, slots, SLOTS_PER_DOT):
            spikes = jnp.concatenate(
                [lhs_of(first + j, interval) for j in range(SLOTS_PER_DOT)], axis=1
            )
            synapses = weights[first : first + SLOTS_PER_DOT].reshape(SLOTS_PER_DOT * 128, 128)
            total = total + jnp.dot(spikes, synapses, preferred_element_type=jnp.float32)
        half = unscale + unscale[: trials // 8 - 4]
        total = total * jnp.concatenate(half + half, axis=0)

        voltage = volt[...]
        fired = []
        for step in range(DMIN):
            voltage = (
                voltage
                - jnp.floor(voltage * scale)
                + total[trials * step : trials * (step + 1)]
                + drive
            )
            flags = voltage >= THRESHOLD
            voltage = jnp.where(flags, 0.0, jnp.maximum(voltage, -THRESHOLD))
            fired.append(flags)
        volt[...] = voltage

        for step in range(DMIN):
            row = jnp.sum(fired[step].astype(jnp.float32), axis=0, keepdims=True)
            counts[pl.ds(interval * DMIN + step, 1), :] = row

        @pl.when(interval < intervals - 1)
        def _():
            store_words(interval + 1, *fired)

        @pl.when(interval == intervals - 1)
        def _():
            per_step = jnp.sum(counts[...], axis=1, keepdims=True).astype(jnp.int32)
            for r in range(WORDS):
                row = jnp.zeros((1, 128), jnp.int32)
                for j in range(4):
                    here = own_lanes & (lanes // AREAS == j)
                    row = jnp.where(here, per_step[4 * r + j : 4 * r + j + 1], row)
                landing[intervals, own_row + r] = row

        exchange(interval + 1)
        return carry

    lax.fori_loop(0, intervals, one_interval, 0)
    out_membrane[...] = volt[...]

    def add_counts(j, total):
        at = (intervals + 2) * per_interval + j * 8 * WORDS
        return total + words[pl.ds(at, 8 * WORDS)]

    summed = lax.fori_loop(
        0, blocks // 8, add_counts, jnp.zeros((8 * WORDS, 1, 128), jnp.int32)
    ).reshape(8, WORDS, 128)
    rates = jnp.sum(summed, axis=0).astype(jnp.float32) / sizes
    for step in range(steps):
        lane0 = AREAS * (step % 4)
        out_rates[step : step + 1] = rates[step // 4 : step // 4 + 1, lane0 : lane0 + AREAS]
    sent = nz - 1 + len(offsets) * nz

    def drain(gather, carry):
        send(gather, 0, sent, z_peer(1), 0, z_sem.at[gather, 0]).wait_send()
        return carry

    lax.fori_loop(0, intervals + 1, drain, 0)


def write_out(membrane, rates, out_membrane, out_rates, sem):
    copies = [
        pltpu.make_async_copy(membrane, out_membrane, sem.at[0]),
        pltpu.make_async_copy(rates, out_rates, sem.at[1]),
    ]
    for copy in copies:
        copy.start()
    for copy in copies:
        copy.wait()


def on_device(
    dims, initial_bits, membrane, drive, leak_shift, weights, pre_block, block_mask, delay, area_of_block
):
    ny, nx, nc, nz, slots, trials, steps = dims
    blocks = ny * nx * nc * nz
    intervals = steps // DMIN
    hbm = pl.BlockSpec(memory_space=pltpu.HBM)
    vmem = pl.BlockSpec(memory_space=pltpu.VMEM)
    shapes = (
        jax.ShapeDtypeStruct((trials, 128), jnp.float32),
        jax.ShapeDtypeStruct((steps, AREAS), jnp.float32),
    )
    run = pl.pallas_call(
        functools.partial(kernel, dims),
        out_shape=shapes,
        in_specs=[hbm] * 9,
        out_specs=(vmem, vmem),
        scratch_shapes=[
            pltpu.VMEM((1, slots), jnp.int32),
            pltpu.VMEM((1, slots), jnp.int32),
            pltpu.VMEM((1, slots), jnp.int32),
            pltpu.VMEM((DMIN, 4, trials), jnp.int32),
            pltpu.VMEM((trials, 128), jnp.float32),
            pltpu.VMEM((1, 128), jnp.int32),
            pltpu.VMEM((1, 128), jnp.int32),
            pltpu.VMEM((1, blocks), jnp.int32),
            pltpu.VMEM((slots, 128, 128), jnp.bfloat16),
            pltpu.VMEM((intervals + 1, blocks * WORDS, 1, 128), jnp.int32),
            pltpu.VMEM(((intervals + 3) * blocks * WORDS, 1, 128), jnp.int32),
            pltpu.VMEM((trials, 128), jnp.float32),
            pltpu.VMEM((16, 128), jnp.float32),
            pltpu.VMEM((4, slots), jnp.int32),
            pltpu.SMEM((4, slots), jnp.int32),
            pltpu.SemaphoreType.DMA((8,)),
            pltpu.SemaphoreType.DMA,
            pltpu.SemaphoreType.DMA,
            pltpu.SemaphoreType.DMA((intervals + 1,)),
            pltpu.SemaphoreType.DMA((intervals + 1, nz - 1)),
            pltpu.SemaphoreType.DMA((intervals + 1, len(batches(nz)))),
        ],
        compiler_params=pltpu.CompilerParams(
            collective_id=0, has_side_effects=True, vmem_limit_bytes=40 << 20
        ),
    )
    operands = (
        pre_block,
        block_mask,
        delay,
        jnp.transpose(initial_bits, (0, 2, 1)),
        membrane,
        drive.reshape(1, 128),
        leak_shift.reshape(1, 128),
        area_of_block.reshape(1, blocks),
        weights.reshape(slots, 128, 128),
    )
    result = run(*[pltpu.with_memory_space_constraint(x, pltpu.HBM) for x in operands])
    return pl.pallas_call(
        write_out,
        out_shape=shapes,
        in_specs=[vmem, vmem],
        out_specs=(hbm, hbm),
        scratch_shapes=[pltpu.SemaphoreType.DMA((2,))],
        compiler_params=pltpu.CompilerParams(vmem_limit_bytes=1 << 20),
    )(*result)


def build(mesh, dims):
    both = ("area", "rank")
    return jax.shard_map(
        functools.partial(on_device, dims),
        mesh=mesh,
        in_specs=(
            P(None, None, both),
            P(None, both),
            P(both),
            P(both),
            P(both, None, None, None),
            P(both, None),
            P(both, None),
            P(both, None),
            P(),
        ),
        out_specs=(P(None, both), P()),
        check_vma=False,
    )


def solution(mesh):
    return build(mesh, (NY, NX, NC, mesh.shape["rank"], 128, 48, STEPS))
```

```python
import functools

import jax
import jax.numpy as jnp
from jax import lax
from jax.experimental import pallas as pl
from jax.experimental.pallas import tpu as pltpu
from jax.sharding import PartitionSpec as P

AREAS = 32
DMIN = 2
STEPS = 10
THRESHOLD = 200.0
MESH = pl.DeviceIdType.MESH
WORDS = 3
SLOTS_PER_DOT = 4
NX, NY, NC = 4, 4, 2


def batches(nz):
    pairs = [(2 * near - 1, 2) for near in range(1, nz // 2)]
    return [(0, 1)] + pairs + [(nz - 1, 1)]


def z_place(offset, nz):
    return 2 * (nz - offset) if offset > nz // 2 else max(2 * offset - 1, 0)


def block_place(area, offset, areas, nz):
    place = jnp.where(offset > nz // 2, 2 * (nz - offset), jnp.maximum(2 * offset - 1, 0))
    single = (place == 0) | (place == nz - 1)
    first = jnp.where(single | (place % 2 == 1), place, place - 1)
    count = jnp.where(single, 1, 2)
    return first * areas + area * count + place - first


def static_row(area, place, areas, nz):
    first, count = next(b for b in batches(nz) if b[0] <= place < b[0] + b[1])
    return (first * areas + area * count + place - first) * WORDS


def ring_hops(step, n):
    return min(step, n - step)


def plane_offsets(ny, nx, nc):
    found = [
        (dy, dx, dc)
        for dy in range(ny)
        for dx in range(nx)
        for dc in range(nc)
        if (dy, dx, dc) != (0, 0, 0)
    ]
    return sorted(found, key=lambda o: -(ring_hops(o[0], ny) + ring_hops(o[1], nx)))


def kernel(
    dims,
    pre_hbm,
    mask_hbm,
    delay_hbm,
    bits_hbm,
    membrane_hbm,
    drive_hbm,
    leak_hbm,
    area_hbm,
    weights_hbm,
    out_membrane,
    out_rates,
    pre_ref,
    mask_ref,
    delay_ref,
    bits_ref,
    membrane_ref,
    drive_ref,
    leak_ref,
    area_ref,
    weights,
    landing,
    words,
    volt,
    counts,
    table_rows,
    table,
    input_sem,
    table_sem,
    weights_sem,
    send_sem,
    z_sem,
    plane_sem,
):
    ny, nx, nc, nz, slots, trials, steps = dims
    areas = ny * nx * nc
    blocks = areas * nz
    per_interval = blocks * WORDS
    intervals = steps // DMIN
    area = lax.axis_index("area")
    rank = lax.axis_index("rank")
    y, x, core = area // (nx * nc), (area // nc) % nx, area % nc
    offsets = plane_offsets(ny, nx, nc)

    def plane_peer(offset):
        dy, dx, dc = offset
        there = (((y + dy) % ny) * nx + (x + dx) % nx) * nc + (core + dc) % nc
        return (there, rank)

    def z_peer(dz):
        return (area, (rank + dz) % nz)

    peers = [z_peer(dz) for dz in range(1, nz)] + [plane_peer(o) for o in offsets]
    barrier = pltpu.get_barrier_semaphore()
    for peer in peers:
        pl.semaphore_signal(barrier, inc=1, device_id=peer, device_id_type=MESH)

    inputs = [
        (pre_hbm, pre_ref),
        (mask_hbm, mask_ref),
        (delay_hbm, delay_ref),
        (bits_hbm, bits_ref),
        (membrane_hbm, membrane_ref),
        (drive_hbm, drive_ref),
        (leak_hbm, leak_ref),
        (area_hbm, area_ref),
    ]
    loads = [
        pltpu.make_async_copy(source, target, input_sem.at[number])
        for number, (source, target) in enumerate(inputs)
    ]
    for load in loads:
        load.start()
    load_weights = pltpu.make_async_copy(weights_hbm, weights, weights_sem)
    load_weights.start()

    def clear(j, carry):
        words[pl.ds(j * 8, 8)] = jnp.zeros((8, 1, 128), jnp.int32)
        return carry

    lax.fori_loop(0, 2 * per_interval // 8, clear, 0)
    counts[...] = jnp.zeros_like(counts)
    for load in loads:
        load.wait()

    pre, keep_slot, d = pre_ref[...], mask_ref[...], delay_ref[...]
    place = block_place(pre // nz, (pre % nz - rank + nz) % nz, areas, nz)
    table_rows[0:1] = keep_slot * (((6 - d) // 2) * per_interval + place * WORDS)
    table_rows[1:2] = keep_slot * (((7 - d) // 2) * per_interval + place * WORDS)
    table_rows[2:3] = keep_slot * per_interval
    table_rows[3:4] = d % 2
    load_table = pltpu.make_async_copy(table_rows, table, table_sem)
    load_table.start()

    sublane = lax.broadcasted_iota(jnp.int32, (8, 128), 0)
    lane = lax.broadcasted_iota(jnp.int32, (trials, 128), 1)
    bit = [jnp.left_shift(jnp.int32(1), sublane + 8 * j) for j in range(4)]
    unscale = [1.0 / b.astype(jnp.float32) for b in bit]

    own_row = static_row(area, 0, areas, nz)

    def groups(fired):
        return [fired[8 * q : 8 * q + 8] for q in range(trials // 8)]

    def fold(parts):
        total = functools.reduce(jnp.bitwise_or, parts)
        return jnp.sum(total, axis=0, keepdims=True)

    def store_words(gather, first, second):
        first, second = groups(first), groups(second)
        zero = jnp.zeros((8, 128), jnp.int32)

        def take(flags, bits):
            return [jnp.where(f, b, zero) for f, b in zip(flags, bits)]

        row = own_row
        landing[gather, row] = fold(take(first[:4], bit))
        landing[gather, row + 1] = fold(take(first[4:], bit[:2]) + take(second[4:], bit[2:]))
        landing[gather, row + 2] = fold(take(second[:4], bit))

    def send(gather, row, count, device, there, semaphore):
        return pltpu.make_async_remote_copy(
            src_ref=landing.at[gather, pl.ds(row, count * WORDS)],
            dst_ref=landing.at[gather, pl.ds(there, count * WORDS)],
            send_sem=send_sem.at[gather],
            recv_sem=semaphore,
            device_id=device,
            device_id_type=MESH,
        )

    def offset_at(place):
        return next(o for o in range(nz) if z_place(o, nz) == place)

    def plane_hops(offset):
        return ring_hops(offset[0], ny) + ring_hops(offset[1], nx)

    def goes_direct(dz, offset):
        hops = ring_hops(dz, nz)
        return hops == 1 or hops + plane_hops(offset) >= ny // 2 + nx // 2 + nz // 2 - 1

    def exchange(gather, with_direct):
        far_first = sorted(range(1, nz), key=lambda dz: -ring_hops(dz, nz))
        for dz in far_first:
            there = static_row(area, z_place(nz - dz, nz), areas, nz)
            send(gather, own_row, 1, z_peer(dz), there, z_sem.at[gather, dz - 1]).start()

        direct = [
            (dz, o) for dz in range(1, nz) for o in offsets if with_direct and goes_direct(dz, o)
        ]
        for dz, offset in sorted(direct, key=lambda p: -(ring_hops(p[0], nz) + plane_hops(p[1]))):
            place = z_place(nz - dz, nz)
            number = next(n for n, (f, c) in enumerate(batches(nz)) if f <= place < f + c)
            device = (plane_peer(offset)[0], z_peer(dz)[1])
            there = static_row(area, place, areas, nz)
            send(gather, own_row, 1, device, there, plane_sem.at[gather, number]).start()

        for number, (first, count) in enumerate(batches(nz)):
            places = range(first, first + count)
            for place in places:
                offset = offset_at(place)
                if offset:
                    row = static_row(area, place, areas, nz)
                    semaphore = z_sem.at[gather, nz - offset - 1]
                    send(gather, row, 1, z_peer(offset), row, semaphore).wait_recv()
            row = static_row(area, first, areas, nz)
            for offset in offsets:
                dz = offset_at(first)
                if not (with_direct and dz and goes_direct(dz, offset)):
                    send(
                        gather, row, count, plane_peer(offset), row, plane_sem.at[gather, number]
                    ).start()

        for number, (first, count) in enumerate(batches(nz)):
            arrived = (areas - 1) * count
            send(gather, 0, arrived, z_peer(1), 0, plane_sem.at[gather, number]).wait_recv()
            rows = areas * count * WORDS
            start = areas * first * WORDS
            step = min(8, areas) * count * WORDS

            def keep(j, carry):
                at = start + j * step
                words[pl.ds((gather + 2) * per_interval + at, step)] = landing[
                    gather, pl.ds(at, step)
                ]
                return carry

            lax.fori_loop(0, rows // step, keep, 0)

    leak = leak_ref[...]
    scale = jnp.ones(leak.shape, jnp.float32)
    for power in range(5):
        on = jnp.bitwise_and(leak, 1 << power) != 0
        scale = scale * jnp.where(on, jnp.float32(2.0 ** -(1 << power)), jnp.float32(1.0))
    drive = drive_ref[...].astype(jnp.float32)
    volt[...] = jnp.floor(membrane_ref[...])

    def initial(step):
        packed = bits_ref[step]
        packed = jnp.concatenate([packed, jnp.zeros((4, trials), jnp.int32)], axis=0)
        packed = jnp.concatenate([packed, jnp.zeros((8, 128 - trials), jnp.int32)], axis=1)
        packed = jnp.transpose(packed)[:trials]
        spread_out = jnp.broadcast_to(packed[:, 0:1], (trials, 128))
        for w in range(1, 4):
            spread_out = jnp.where(
                lane >= 32 * w, jnp.broadcast_to(packed[:, w : w + 1], (trials, 128)), spread_out
            )
        picked = jnp.bitwise_and(jnp.right_shift(spread_out, jnp.bitwise_and(lane, 31)), 1)
        return picked != 0

    store_words(0, initial(0), initial(1))
    lane_area = lax.broadcasted_iota(jnp.int32, (128, blocks), 0) % AREAS
    belongs = (jnp.broadcast_to(area_ref[...], (128, blocks)) == lane_area).astype(jnp.float32)
    sizes = lax.dot_general(
        jnp.ones((8, blocks), jnp.float32),
        belongs,
        (((1,), (1,)), ((), ())),
        precision=lax.Precision.HIGHEST,
        preferred_element_type=jnp.float32,
    )[0:1] * float(trials * 128)
    block_lane = lax.broadcasted_iota(jnp.int32, (1, blocks), 1)
    own_area = jnp.sum(
        jnp.where(block_lane == area * nz + rank, area_ref[...], 0), axis=1, keepdims=True
    )
    lanes = lax.broadcasted_iota(jnp.int32, (1, 128), 1)
    own_lanes = lanes % AREAS == own_area
    pl.semaphore_wait(barrier, len(peers))
    exchange(0, False)
    load_weights.wait()
    load_table.wait()

    def lhs_of(k, interval):
        s = table[3, k]
        row0 = table[0, k] + interval * table[2, k]
        row1 = table[1, k] + interval * table[2, k]
        w0 = words[row0 + 2 * s]
        w1 = jnp.right_shift(words[row0 + 1], 16 * s)
        w2 = words[row1 + 2 * (1 - s)]
        w3 = jnp.right_shift(words[row1 + 1], 16 * (1 - s))
        parts = []
        for wide, narrow in ((w0, w1), (w2, w3)):
            wide = jnp.broadcast_to(wide, (8, 128))
            narrow = jnp.broadcast_to(narrow, (8, 128))
            parts += [jnp.bitwise_and(wide, b) for b in bit]
            parts += [jnp.bitwise_and(narrow, b) for b in bit[: trials // 8 - 4]]
        return jnp.concatenate(parts, axis=0).astype(jnp.float32).astype(jnp.bfloat16)

    def one_interval(interval, carry):
        total = jnp.zeros((2 * trials, 128), jnp.float32)
        for first in range(0, slots, SLOTS_PER_DOT):
            spikes = jnp.concatenate(
                [lhs_of(first + j, interval) for j in range(SLOTS_PER_DOT)], axis=1
            )
            synapses = weights[first : first + SLOTS_PER_DOT].reshape(SLOTS_PER_DOT * 128, 128)
            total = total + jnp.dot(spikes, synapses, preferred_element_type=jnp.float32)
        half = unscale + unscale[: trials // 8 - 4]
        total = total * jnp.concatenate(half + half, axis=0)

        voltage = volt[...]
        fired = []
        for step in range(DMIN):
            voltage = (
                voltage
                - jnp.floor(voltage * scale)
                + total[trials * step : trials * (step + 1)]
                + drive
            )
            flags = voltage >= THRESHOLD
            voltage = jnp.where(flags, 0.0, jnp.maximum(voltage, -THRESHOLD))
            fired.append(flags)
        volt[...] = voltage

        for step in range(DMIN):
            row = jnp.sum(fired[step].astype(jnp.float32), axis=0, keepdims=True)
            counts[pl.ds(interval * DMIN + step, 1), :] = row

        @pl.when(interval < intervals - 1)
        def _():
            store_words(interval + 1, *fired)

        @pl.when(interval == intervals - 1)
        def _():
            per_step = jnp.sum(counts[...], axis=1, keepdims=True).astype(jnp.int32)
            for r in range(WORDS):
                row = jnp.zeros((1, 128), jnp.int32)
                for j in range(4):
                    here = own_lanes & (lanes // AREAS == j)
                    row = jnp.where(here, per_step[4 * r + j : 4 * r + j + 1], row)
                landing[intervals, own_row + r] = row

        exchange(interval + 1, True)
        return carry

    lax.fori_loop(0, intervals, one_interval, 0)
    out_membrane[...] = volt[...]

    def add_counts(j, total):
        at = (intervals + 2) * per_interval + j * 8 * WORDS
        return total + words[pl.ds(at, 8 * WORDS)]

    summed = lax.fori_loop(
        0, blocks // 8, add_counts, jnp.zeros((8 * WORDS, 1, 128), jnp.int32)
    ).reshape(8, WORDS, 128)
    rates = jnp.sum(summed, axis=0).astype(jnp.float32) / sizes
    for step in range(steps):
        lane0 = AREAS * (step % 4)
        out_rates[step : step + 1] = rates[step // 4 : step // 4 + 1, lane0 : lane0 + AREAS]
    sent = nz - 1 + len(offsets) * nz

    def drain(gather, carry):
        send(gather, 0, sent, z_peer(1), 0, z_sem.at[gather, 0]).wait_send()
        return carry

    lax.fori_loop(0, intervals + 1, drain, 0)


def write_out(membrane, rates, out_membrane, out_rates, sem):
    copies = [
        pltpu.make_async_copy(membrane, out_membrane, sem.at[0]),
        pltpu.make_async_copy(rates, out_rates, sem.at[1]),
    ]
    for copy in copies:
        copy.start()
    for copy in copies:
        copy.wait()


def on_device(
    dims, initial_bits, membrane, drive, leak_shift, weights, pre_block, block_mask, delay, area_of_block
):
    ny, nx, nc, nz, slots, trials, steps = dims
    blocks = ny * nx * nc * nz
    intervals = steps // DMIN
    hbm = pl.BlockSpec(memory_space=pltpu.HBM)
    vmem = pl.BlockSpec(memory_space=pltpu.VMEM)
    shapes = (
        jax.ShapeDtypeStruct((trials, 128), jnp.float32),
        jax.ShapeDtypeStruct((steps, AREAS), jnp.float32),
    )
    run = pl.pallas_call(
        functools.partial(kernel, dims),
        out_shape=shapes,
        in_specs=[hbm] * 9,
        out_specs=(vmem, vmem),
        scratch_shapes=[
            pltpu.VMEM((1, slots), jnp.int32),
            pltpu.VMEM((1, slots), jnp.int32),
            pltpu.VMEM((1, slots), jnp.int32),
            pltpu.VMEM((DMIN, 4, trials), jnp.int32),
            pltpu.VMEM((trials, 128), jnp.float32),
            pltpu.VMEM((1, 128), jnp.int32),
            pltpu.VMEM((1, 128), jnp.int32),
            pltpu.VMEM((1, blocks), jnp.int32),
            pltpu.VMEM((slots, 128, 128), jnp.bfloat16),
            pltpu.VMEM((intervals + 1, blocks * WORDS, 1, 128), jnp.int32),
            pltpu.VMEM(((intervals + 3) * blocks * WORDS, 1, 128), jnp.int32),
            pltpu.VMEM((trials, 128), jnp.float32),
            pltpu.VMEM((16, 128), jnp.float32),
            pltpu.VMEM((4, slots), jnp.int32),
            pltpu.SMEM((4, slots), jnp.int32),
            pltpu.SemaphoreType.DMA((8,)),
            pltpu.SemaphoreType.DMA,
            pltpu.SemaphoreType.DMA,
            pltpu.SemaphoreType.DMA((intervals + 1,)),
            pltpu.SemaphoreType.DMA((intervals + 1, nz - 1)),
            pltpu.SemaphoreType.DMA((intervals + 1, len(batches(nz)))),
        ],
        compiler_params=pltpu.CompilerParams(
            collective_id=0, has_side_effects=True, vmem_limit_bytes=40 << 20
        ),
    )
    operands = (
        pre_block,
        block_mask,
        delay,
        jnp.transpose(initial_bits, (0, 2, 1)),
        membrane,
        drive.reshape(1, 128),
        leak_shift.reshape(1, 128),
        area_of_block.reshape(1, blocks),
        weights.reshape(slots, 128, 128),
    )
    result = run(*[pltpu.with_memory_space_constraint(x, pltpu.HBM) for x in operands])
    return pl.pallas_call(
        write_out,
        out_shape=shapes,
        in_specs=[vmem, vmem],
        out_specs=(hbm, hbm),
        scratch_shapes=[pltpu.SemaphoreType.DMA((2,))],
        compiler_params=pltpu.CompilerParams(vmem_limit_bytes=1 << 20),
    )(*result)


def build(mesh, dims):
    both = ("area", "rank")
    return jax.shard_map(
        functools.partial(on_device, dims),
        mesh=mesh,
        in_specs=(
            P(None, None, both),
            P(None, both),
            P(both),
            P(both),
            P(both, None, None, None),
            P(both, None),
            P(both, None),
            P(both, None),
            P(),
        ),
        out_specs=(P(None, both), P()),
        check_vma=False,
    )


def solution(mesh):
    return build(mesh, (NY, NX, NC, mesh.shape["rank"], 128, 48, STEPS))
```

```python
import functools

import jax
import jax.numpy as jnp
from jax import lax
from jax.experimental import pallas as pl
from jax.experimental.pallas import tpu as pltpu
from jax.sharding import PartitionSpec as P

AREAS = 32
DMIN = 2
STEPS = 10
THRESHOLD = 200.0
MESH = pl.DeviceIdType.MESH
WORDS = 3
SLOTS_PER_DOT = 4
NX, NY, NC = 4, 4, 2


def batches(nz):
    pairs = [(2 * near - 1, 2) for near in range(1, nz // 2)]
    return [(0, 1)] + pairs + [(nz - 1, 1)]


def z_place(offset, nz):
    return 2 * (nz - offset) if offset > nz // 2 else max(2 * offset - 1, 0)


def core_major(area, areas):
    return (area % NC) * (areas // NC) + area // NC


def block_place(area, offset, areas, nz):
    area = core_major(area, areas)
    place = jnp.where(offset > nz // 2, 2 * (nz - offset), jnp.maximum(2 * offset - 1, 0))
    single = (place == 0) | (place == nz - 1)
    first = jnp.where(single | (place % 2 == 1), place, place - 1)
    count = jnp.where(single, 1, 2)
    return first * areas + area * count + place - first


def static_row(area, place, areas, nz):
    area = core_major(area, areas)
    first, count = next(b for b in batches(nz) if b[0] <= place < b[0] + b[1])
    return (first * areas + area * count + place - first) * WORDS


def ring_hops(step, n):
    return min(step, n - step)


def plane_offsets(ny, nx, nc):
    found = [
        (dy, dx, dc)
        for dy in range(ny)
        for dx in range(nx)
        for dc in range(nc)
        if (dy, dx, dc) != (0, 0, 0)
    ]
    return sorted(found, key=lambda o: -(ring_hops(o[0], ny) + ring_hops(o[1], nx)))


def kernel(
    dims,
    pre_hbm,
    mask_hbm,
    delay_hbm,
    bits_hbm,
    membrane_hbm,
    drive_hbm,
    leak_hbm,
    area_hbm,
    weights_hbm,
    out_membrane,
    out_rates,
    pre_ref,
    mask_ref,
    delay_ref,
    bits_ref,
    membrane_ref,
    drive_ref,
    leak_ref,
    area_ref,
    weights,
    landing,
    words,
    volt,
    counts,
    table_rows,
    table,
    input_sem,
    table_sem,
    weights_sem,
    send_sem,
    z_sem,
    plane_sem,
    twin_sem,
):
    ny, nx, nc, nz, slots, trials, steps = dims
    areas = ny * nx * nc
    blocks = areas * nz
    per_interval = blocks * WORDS
    intervals = steps // DMIN
    area = lax.axis_index("area")
    rank = lax.axis_index("rank")
    y, x, core = area // (nx * nc), (area // nc) % nx, area % nc
    offsets = plane_offsets(ny, nx, nc)

    def plane_peer(offset):
        dy, dx, dc = offset
        there = (((y + dy) % ny) * nx + (x + dx) % nx) * nc + (core + dc) % nc
        return (there, rank)

    def z_peer(dz):
        return (area, (rank + dz) % nz)

    peers = [z_peer(dz) for dz in range(1, nz)] + [plane_peer(o) for o in offsets]
    barrier = pltpu.get_barrier_semaphore()
    for peer in peers:
        pl.semaphore_signal(barrier, inc=1, device_id=peer, device_id_type=MESH)

    inputs = [
        (pre_hbm, pre_ref),
        (mask_hbm, mask_ref),
        (delay_hbm, delay_ref),
        (bits_hbm, bits_ref),
        (membrane_hbm, membrane_ref),
        (drive_hbm, drive_ref),
        (leak_hbm, leak_ref),
        (area_hbm, area_ref),
    ]
    loads = [
        pltpu.make_async_copy(source, target, input_sem.at[number])
        for number, (source, target) in enumerate(inputs)
    ]
    for load in loads:
        load.start()
    load_weights = pltpu.make_async_copy(weights_hbm, weights, weights_sem)
    load_weights.start()

    def clear(j, carry):
        words[pl.ds(j * 8, 8)] = jnp.zeros((8, 1, 128), jnp.int32)
        return carry

    lax.fori_loop(0, 2 * per_interval // 8, clear, 0)
    counts[...] = jnp.zeros_like(counts)
    for load in loads:
        load.wait()

    pre, keep_slot, d = pre_ref[...], mask_ref[...], delay_ref[...]
    place = block_place(pre // nz, (pre % nz - rank + nz) % nz, areas, nz)
    table_rows[0:1] = keep_slot * (((6 - d) // 2) * per_interval + place * WORDS)
    table_rows[1:2] = keep_slot * (((7 - d) // 2) * per_interval + place * WORDS)
    table_rows[2:3] = keep_slot * per_interval
    table_rows[3:4] = d % 2
    load_table = pltpu.make_async_copy(table_rows, table, table_sem)
    load_table.start()

    sublane = lax.broadcasted_iota(jnp.int32, (8, 128), 0)
    lane = lax.broadcasted_iota(jnp.int32, (trials, 128), 1)
    bit = [jnp.left_shift(jnp.int32(1), sublane + 8 * j) for j in range(4)]
    unscale = [1.0 / b.astype(jnp.float32) for b in bit]

    own_row = static_row(area, 0, areas, nz)

    def groups(fired):
        return [fired[8 * q : 8 * q + 8] for q in range(trials // 8)]

    def fold(parts):
        total = functools.reduce(jnp.bitwise_or, parts)
        return jnp.sum(total, axis=0, keepdims=True)

    def store_words(gather, first, second):
        first, second = groups(first), groups(second)
        zero = jnp.zeros((8, 128), jnp.int32)

        def take(flags, bits):
            return [jnp.where(f, b, zero) for f, b in zip(flags, bits)]

        row = own_row
        landing[gather, row] = fold(take(first[:4], bit))
        landing[gather, row + 1] = fold(take(first[4:], bit[:2]) + take(second[4:], bit[2:]))
        landing[gather, row + 2] = fold(take(second[:4], bit))

    def send(gather, row, count, device, there, semaphore):
        return pltpu.make_async_remote_copy(
            src_ref=landing.at[gather, pl.ds(row, count * WORDS)],
            dst_ref=landing.at[gather, pl.ds(there, count * WORDS)],
            send_sem=send_sem.at[gather],
            recv_sem=semaphore,
            device_id=device,
            device_id_type=MESH,
        )

    def offset_at(place):
        return next(o for o in range(nz) if z_place(o, nz) == place)

    def plane_hops(offset):
        return ring_hops(offset[0], ny) + ring_hops(offset[1], nx)

    def by_twin(dz):
        return ring_hops(dz, nz) <= nz // 4

    def goes_direct(dz, offset):
        far = ring_hops(dz, nz) + plane_hops(offset) >= ny // 2 + nx // 2 + nz // 2 - 1
        return by_twin(dz) or far

    def plane_of(dz):
        return [o for o in offsets if o[2] == 0] if by_twin(dz) else offsets

    def exchange(gather, with_direct):
        far_first = sorted(range(1, nz), key=lambda dz: -ring_hops(dz, nz))
        for dz in far_first:
            there = static_row(area, z_place(nz - dz, nz), areas, nz)
            send(gather, own_row, 1, z_peer(dz), there, z_sem.at[gather, dz - 1]).start()

        direct = [
            (dz, o)
            for dz in range(1, nz)
            for o in plane_of(dz)
            if with_direct and goes_direct(dz, o)
        ]
        for dz, offset in sorted(direct, key=lambda p: -(ring_hops(p[0], nz) + plane_hops(p[1]))):
            place = z_place(nz - dz, nz)
            number = next(n for n, (f, c) in enumerate(batches(nz)) if f <= place < f + c)
            device = (plane_peer(offset)[0], z_peer(dz)[1])
            there = static_row(area, place, areas, nz)
            send(gather, own_row, 1, device, there, plane_sem.at[gather, number]).start()

        for number, (first, count) in enumerate(batches(nz)):
            places = range(first, first + count)
            for place in places:
                offset = offset_at(place)
                if offset:
                    row = static_row(area, place, areas, nz)
                    semaphore = z_sem.at[gather, nz - offset - 1]
                    send(gather, row, 1, z_peer(offset), row, semaphore).wait_recv()
            row = static_row(area, first, areas, nz)
            dz = offset_at(first)
            for offset in plane_of(dz):
                if not (with_direct and dz and goes_direct(dz, offset)):
                    send(
                        gather, row, count, plane_peer(offset), row, plane_sem.at[gather, number]
                    ).start()

        half = areas // nc

        def wait_plane(number, blocks_in):
            send(gather, 0, blocks_in, z_peer(1), 0, plane_sem.at[gather, number]).wait_recv()

        for number, (first, count) in enumerate(batches(nz)):
            if by_twin(offset_at(first)):
                wait_plane(number, (half - 1) * count)
                row = (first * areas + core * half * count) * WORDS
                semaphore = twin_sem.at[gather, number]
                send(gather, row, half * count, plane_peer((0, 0, 1)), row, semaphore).start()

        for number, (first, count) in enumerate(batches(nz)):
            if by_twin(offset_at(first)):
                semaphore = twin_sem.at[gather, number]
                send(gather, 0, half * count, z_peer(1), 0, semaphore).wait_recv()
            else:
                wait_plane(number, (areas - 1) * count)
            rows = areas * count * WORDS
            start = areas * first * WORDS
            step = min(8, areas) * count * WORDS

            def keep(j, carry):
                at = start + j * step
                words[pl.ds((gather + 2) * per_interval + at, step)] = landing[
                    gather, pl.ds(at, step)
                ]
                return carry

            lax.fori_loop(0, rows // step, keep, 0)

    leak = leak_ref[...]
    scale = jnp.ones(leak.shape, jnp.float32)
    for power in range(5):
        on = jnp.bitwise_and(leak, 1 << power) != 0
        scale = scale * jnp.where(on, jnp.float32(2.0 ** -(1 << power)), jnp.float32(1.0))
    drive = drive_ref[...].astype(jnp.float32)
    volt[...] = jnp.floor(membrane_ref[...])

    def initial(step):
        packed = bits_ref[step]
        packed = jnp.concatenate([packed, jnp.zeros((4, trials), jnp.int32)], axis=0)
        packed = jnp.concatenate([packed, jnp.zeros((8, 128 - trials), jnp.int32)], axis=1)
        packed = jnp.transpose(packed)[:trials]
        spread_out = jnp.broadcast_to(packed[:, 0:1], (trials, 128))
        for w in range(1, 4):
            spread_out = jnp.where(
                lane >= 32 * w, jnp.broadcast_to(packed[:, w : w + 1], (trials, 128)), spread_out
            )
        picked = jnp.bitwise_and(jnp.right_shift(spread_out, jnp.bitwise_and(lane, 31)), 1)
        return picked != 0

    store_words(0, initial(0), initial(1))
    lane_area = lax.broadcasted_iota(jnp.int32, (128, blocks), 0) % AREAS
    belongs = (jnp.broadcast_to(area_ref[...], (128, blocks)) == lane_area).astype(jnp.float32)
    sizes = lax.dot_general(
        jnp.ones((8, blocks), jnp.float32),
        belongs,
        (((1,), (1,)), ((), ())),
        precision=lax.Precision.HIGHEST,
        preferred_element_type=jnp.float32,
    )[0:1] * float(trials * 128)
    block_lane = lax.broadcasted_iota(jnp.int32, (1, blocks), 1)
    own_area = jnp.sum(
        jnp.where(block_lane == area * nz + rank, area_ref[...], 0), axis=1, keepdims=True
    )
    lanes = lax.broadcasted_iota(jnp.int32, (1, 128), 1)
    own_lanes = lanes % AREAS == own_area
    pl.semaphore_wait(barrier, len(peers))
    exchange(0, False)
    load_weights.wait()
    load_table.wait()

    def lhs_of(k, interval):
        s = table[3, k]
        row0 = table[0, k] + interval * table[2, k]
        row1 = table[1, k] + interval * table[2, k]
        w0 = words[row0 + 2 * s]
        w1 = jnp.right_shift(words[row0 + 1], 16 * s)
        w2 = words[row1 + 2 * (1 - s)]
        w3 = jnp.right_shift(words[row1 + 1], 16 * (1 - s))
        parts = []
        for wide, narrow in ((w0, w1), (w2, w3)):
            wide = jnp.broadcast_to(wide, (8, 128))
            narrow = jnp.broadcast_to(narrow, (8, 128))
            parts += [jnp.bitwise_and(wide, b) for b in bit]
            parts += [jnp.bitwise_and(narrow, b) for b in bit[: trials // 8 - 4]]
        return jnp.concatenate(parts, axis=0).astype(jnp.float32).astype(jnp.bfloat16)

    def one_interval(interval, carry):
        total = jnp.zeros((2 * trials, 128), jnp.float32)
        for first in range(0, slots, SLOTS_PER_DOT):
            spikes = jnp.concatenate(
                [lhs_of(first + j, interval) for j in range(SLOTS_PER_DOT)], axis=1
            )
            synapses = weights[first : first + SLOTS_PER_DOT].reshape(SLOTS_PER_DOT * 128, 128)
            total = total + jnp.dot(spikes, synapses, preferred_element_type=jnp.float32)
        half = unscale + unscale[: trials // 8 - 4]
        total = total * jnp.concatenate(half + half, axis=0)

        voltage = volt[...]
        fired = []
        for step in range(DMIN):
            voltage = (
                voltage
                - jnp.floor(voltage * scale)
                + total[trials * step : trials * (step + 1)]
                + drive
            )
            flags = voltage >= THRESHOLD
            voltage = jnp.where(flags, 0.0, jnp.maximum(voltage, -THRESHOLD))
            fired.append(flags)
        volt[...] = voltage

        for step in range(DMIN):
            row = jnp.sum(fired[step].astype(jnp.float32), axis=0, keepdims=True)
            counts[pl.ds(interval * DMIN + step, 1), :] = row

        @pl.when(interval < intervals - 1)
        def _():
            store_words(interval + 1, *fired)

        @pl.when(interval == intervals - 1)
        def _():
            per_step = jnp.sum(counts[...], axis=1, keepdims=True).astype(jnp.int32)
            for r in range(WORDS):
                row = jnp.zeros((1, 128), jnp.int32)
                for j in range(4):
                    here = own_lanes & (lanes // AREAS == j)
                    row = jnp.where(here, per_step[4 * r + j : 4 * r + j + 1], row)
                landing[intervals, own_row + r] = row

        exchange(interval + 1, True)
        return carry

    lax.fori_loop(0, intervals, one_interval, 0)
    out_membrane[...] = volt[...]

    def add_counts(j, total):
        at = (intervals + 2) * per_interval + j * 8 * WORDS
        return total + words[pl.ds(at, 8 * WORDS)]

    summed = lax.fori_loop(
        0, blocks // 8, add_counts, jnp.zeros((8 * WORDS, 1, 128), jnp.int32)
    ).reshape(8, WORDS, 128)
    rates = jnp.sum(summed, axis=0).astype(jnp.float32) / sizes
    for step in range(steps):
        lane0 = AREAS * (step % 4)
        out_rates[step : step + 1] = rates[step // 4 : step // 4 + 1, lane0 : lane0 + AREAS]
    sent = blocks - 1

    def drain(gather, carry):
        send(gather, 0, sent, z_peer(1), 0, z_sem.at[gather, 0]).wait_send()
        return carry

    lax.fori_loop(0, intervals + 1, drain, 0)


def write_out(membrane, rates, out_membrane, out_rates, sem):
    copies = [
        pltpu.make_async_copy(membrane, out_membrane, sem.at[0]),
        pltpu.make_async_copy(rates, out_rates, sem.at[1]),
    ]
    for copy in copies:
        copy.start()
    for copy in copies:
        copy.wait()


def on_device(
    dims, initial_bits, membrane, drive, leak_shift, weights, pre_block, block_mask, delay, area_of_block
):
    ny, nx, nc, nz, slots, trials, steps = dims
    blocks = ny * nx * nc * nz
    intervals = steps // DMIN
    hbm = pl.BlockSpec(memory_space=pltpu.HBM)
    vmem = pl.BlockSpec(memory_space=pltpu.VMEM)
    shapes = (
        jax.ShapeDtypeStruct((trials, 128), jnp.float32),
        jax.ShapeDtypeStruct((steps, AREAS), jnp.float32),
    )
    run = pl.pallas_call(
        functools.partial(kernel, dims),
        out_shape=shapes,
        in_specs=[hbm] * 9,
        out_specs=(vmem, vmem),
        scratch_shapes=[
            pltpu.VMEM((1, slots), jnp.int32),
            pltpu.VMEM((1, slots), jnp.int32),
            pltpu.VMEM((1, slots), jnp.int32),
            pltpu.VMEM((DMIN, 4, trials), jnp.int32),
            pltpu.VMEM((trials, 128), jnp.float32),
            pltpu.VMEM((1, 128), jnp.int32),
            pltpu.VMEM((1, 128), jnp.int32),
            pltpu.VMEM((1, blocks), jnp.int32),
            pltpu.VMEM((slots, 128, 128), jnp.bfloat16),
            pltpu.VMEM((intervals + 1, blocks * WORDS, 1, 128), jnp.int32),
            pltpu.VMEM(((intervals + 3) * blocks * WORDS, 1, 128), jnp.int32),
            pltpu.VMEM((trials, 128), jnp.float32),
            pltpu.VMEM((16, 128), jnp.float32),
            pltpu.VMEM((4, slots), jnp.int32),
            pltpu.SMEM((4, slots), jnp.int32),
            pltpu.SemaphoreType.DMA((8,)),
            pltpu.SemaphoreType.DMA,
            pltpu.SemaphoreType.DMA,
            pltpu.SemaphoreType.DMA((intervals + 1,)),
            pltpu.SemaphoreType.DMA((intervals + 1, nz - 1)),
            pltpu.SemaphoreType.DMA((intervals + 1, len(batches(nz)))),
            pltpu.SemaphoreType.DMA((intervals + 1, len(batches(nz)))),
        ],
        compiler_params=pltpu.CompilerParams(
            collective_id=0, has_side_effects=True, vmem_limit_bytes=40 << 20
        ),
    )
    operands = (
        pre_block,
        block_mask,
        delay,
        jnp.transpose(initial_bits, (0, 2, 1)),
        membrane,
        drive.reshape(1, 128),
        leak_shift.reshape(1, 128),
        area_of_block.reshape(1, blocks),
        weights.reshape(slots, 128, 128),
    )
    result = run(*[pltpu.with_memory_space_constraint(x, pltpu.HBM) for x in operands])
    return pl.pallas_call(
        write_out,
        out_shape=shapes,
        in_specs=[vmem, vmem],
        out_specs=(hbm, hbm),
        scratch_shapes=[pltpu.SemaphoreType.DMA((2,))],
        compiler_params=pltpu.CompilerParams(vmem_limit_bytes=1 << 20),
    )(*result)


def build(mesh, dims):
    both = ("area", "rank")
    return jax.shard_map(
        functools.partial(on_device, dims),
        mesh=mesh,
        in_specs=(
            P(None, None, both),
            P(None, both),
            P(both),
            P(both),
            P(both, None, None, None),
            P(both, None),
            P(both, None),
            P(both, None),
            P(),
        ),
        out_specs=(P(None, both), P()),
        check_vma=False,
    )


def solution(mesh):
    return build(mesh, (NY, NX, NC, mesh.shape["rank"], 128, 48, STEPS))
```
